32 devices in a mesh: slab: 2 (over x), grp: 16 (over z, y, core).
Axes of the slice: x: 2, y: 2, z: 4, core: 2. Of those that a mesh axis runs over, the one named last changes fastest.
Arguments:
- blocks: bfloat16 [128, 9, 256, 256], P(('slab', 'grp')), may hold values from -0.75 to 0.75
- diag_shift: float32 [32768], P(('slab', 'grp')), may hold values from 1 to 16
- offsets: int32 [128, 2], P(('slab', 'grp')), may hold values from 0 to 4
Outputs:
- factors: bfloat16 [128, 9, 256, 256], P(('slab', 'grp'))
The draws below stay inside these ranges and needn't reach their ends.
Inputs may be any that keep to these rules, and one draw needn't show every extreme that they name: offsets[i, 0] bounds from above the pattern's blocks left of the diagonal block of block row i and offsets[i, 1] those right of it; blocks that would lie outside the matrix are not in the pattern.
All inputs are finite; a program needn't handle non-finite values.
Results may differ from the reference program's by a relative error of at most 0.001.
Values may be sent and summed in bfloat16 or wider, within the bound.
No kernel may reach another device: no remote copies, remote signals or barrier semaphores. Data moves between devices by JAX's collectives and lax.ppermute only.
A program may use at most 256 MiB of HBM per device.

```python
import math
import jax
import jax.numpy as jnp
from jax import lax

B = 256
BW = 4
RB = 4
ITERS = 2
NBR = 128
N_SLAB = 2
N_GRP = 16


def touch_ends(drawn, rng, least, high):
    place = [jax.random.randint(jax.random.fold_in(rng, axis), (), 0, length) for axis, length in enumerate(drawn.shape)]
    main_axis = drawn.shape.index(max(drawn.shape))
    next_to = place[:main_axis] + [(place[main_axis] + 1) % drawn.shape[main_axis]] + place[main_axis + 1:]
    return drawn.at[tuple(place)].set(least).at[tuple(next_to)].set(high)


def steps_of(stream_key, dims, split, low, largest):
    level, own = 1.0, jax.random.fold_in(stream_key, 6)
    for dim, blocks in split:
        steps = jnp.exp(jax.random.uniform(jax.random.fold_in(own, dim), (blocks,), jnp.float32, low / len(split), largest / len(split)))
        level = level * jnp.repeat(steps, dims[dim] // blocks).reshape([-1 if axis == dim else 1 for axis in range(len(dims))])
    return level


def bell_draw(rng, dims, width, reach, split=(), held_as=jnp.bfloat16):
    gain = steps_of(rng, dims, split, -0.22, 0.18) if split else 1.0
    drawn = jax.random.normal(rng, dims, jnp.float32) * width * gain
    return jnp.minimum(jnp.maximum(drawn, -reach), reach).astype(held_as)


def setup_inputs(seed: int = 0) -> dict:
    key_of = jax.random.split(jax.random.key(seed), 4)
    return {
        "blocks": bell_draw(key_of[0], (NBR, 2 * BW + 1, B, B), 0.05, 0.75, ((0, 32),)),
        "diag_shift": jnp.clip(jnp.exp(math.log(16.0) - 2.7725887 * jax.random.uniform(key_of[1], (NBR * B,), jnp.float32) ** steps_of(key_of[1], (NBR * B,), ((0, 32),), -0.2, 0.2)), 1.0, 16.0),
        "offsets": touch_ends(jax.random.randint(key_of[2], (NBR, 2), 0, BW + 1), jax.random.fold_in(key_of[2], 1), 0, BW).astype(jnp.int32),
    }


def band_pattern(global_rows, offsets, band_count, all_rows):
    band_reach = (band_count - 1) // 2
    relative = jnp.arange(band_count, dtype=jnp.int32) - band_reach
    lower_count = offsets[:, 0:1]
    upper_count = offsets[:, 1:2]
    target = global_rows[:, None] + relative[None, :]
    left_side = (relative < 0) & (-relative <= lower_count) & (target >= 0)
    right_side = (relative > 0) & (relative <= upper_count) & (target < all_rows)
    return (relative == 0) | left_side | right_side

def new_rows(factors_now, above_rows, scaled, present):
    band_count = factors_now.shape[1]
    band_reach = (band_count - 1) // 2
    row_count = factors_now.shape[0]
    block_size = factors_now.shape[2]
    partial_value = scaled.astype(jnp.float32)
    for offset_back in range(1, band_reach + 1):
        left_block = factors_now[:, band_reach - offset_back].astype(jnp.float32)
        upper_rows = above_rows[band_reach - offset_back:band_reach - offset_back + row_count, 1:].astype(jnp.float32)
        product = jnp.einsum('rab,rsbc->rsac', left_block, upper_rows)
        partial_value = partial_value.at[:, band_reach - offset_back + 1:2 * band_reach - offset_back + 1].add(-product)
    pieces = []
    for offset_back in range(band_reach, 0, -1):
        pivot_block = above_rows[band_reach - offset_back:band_reach - offset_back + row_count, 0].astype(jnp.float32)
        strict = jnp.triu(pivot_block, 1)
        inner_term = jnp.einsum('rab,rbc->rac', factors_now[:, band_reach - offset_back].astype(jnp.float32), strict)
        diag_values = jnp.diagonal(pivot_block, axis1=1, axis2=2)
        divisor = jnp.where(present[:, band_reach - offset_back][:, None], diag_values, 1.0)
        pieces.append((partial_value[:, band_reach - offset_back] - inner_term) / divisor[:, None, :])
    own_block = factors_now[:, band_reach].astype(jnp.float32)
    strict_lower = jnp.tril(own_block, -1)
    diag_rest = partial_value[:, band_reach] - jnp.einsum('rab,rbc->rac', strict_lower, jnp.triu(own_block, 1))
    own_diag = jnp.diagonal(own_block, axis1=1, axis2=2)
    below_mask = jnp.tril(jnp.ones((block_size, block_size), jnp.int32), -1) > 0
    pieces.append(jnp.where(below_mask[None], diag_rest / own_diag[:, None, :], diag_rest))
    upper_terms = partial_value[:, band_reach + 1:] - jnp.einsum('rab,rsbc->rsac', strict_lower, factors_now[:, band_reach + 1:].astype(jnp.float32))
    stacked = jnp.concatenate([jnp.stack(pieces, 1), upper_terms], 1)
    return jnp.where(present[:, :, None, None], stacked, 0.0).astype(jnp.bfloat16)

def reference(blocks, diag_shift, offsets):
    row_total, band_count, block_size, _ = blocks.shape
    band_reach = (band_count - 1) // 2
    shift_rows = diag_shift.reshape(row_total, block_size)
    diag_values = shift_rows + jnp.diagonal(blocks[:, band_reach].astype(jnp.float32), axis1=1, axis2=2)
    padded = jnp.pad(diag_values, ((band_reach, band_reach), (0, 0)))
    positive = padded > 0
    scales = jnp.where(positive, 1.0 / jnp.sqrt(jnp.where(positive, padded, 1.0)), 0.0)
    row_scale = scales[band_reach:band_reach + row_total]
    col_scale = jnp.stack([scales[column:column + row_total] for column in range(band_count)], 1)
    present = band_pattern(jnp.arange(row_total, dtype=jnp.int32), offsets, band_count, row_total)
    group_count = row_total // RB
    identity = jnp.eye(block_size, dtype=jnp.float32)

    def scale_group(index):
        start = (index * RB).astype(jnp.int32)
        piece = lax.dynamic_slice_in_dim(blocks, start, RB, 0).astype(jnp.float32)
        added = lax.dynamic_slice_in_dim(shift_rows, start, RB, 0)
        piece = piece.at[:, band_reach].add(identity[None] * added[:, None, :])
        rscale = lax.dynamic_slice_in_dim(row_scale, start, RB, 0)
        cscale = lax.dynamic_slice_in_dim(col_scale, start, RB, 0)
        marks = lax.dynamic_slice_in_dim(present, start, RB, 0)
        value = piece * rscale[:, None, :, None] * cscale[:, :, None, :]
        return jnp.where(marks[:, :, None, None], value, 0.0).astype(jnp.bfloat16)
    scaled = lax.map(scale_group, jnp.arange(group_count, dtype=jnp.int32)).reshape(blocks.shape)
    padded_state = jnp.concatenate([jnp.zeros((band_reach,) + blocks.shape[1:], jnp.bfloat16), scaled], 0)
    slab_rows = N_GRP * RB

    def slab_update(slab_index, padded_state):
        slab_start = (slab_index * slab_rows).astype(jnp.int32)

        def group_update(group_index):
            start = (slab_start + group_index * RB).astype(jnp.int32)
            current = lax.dynamic_slice_in_dim(padded_state, start + band_reach, RB, 0)
            above_rows = lax.dynamic_slice_in_dim(padded_state, start, RB + band_reach, 0)[:, band_reach:]
            return new_rows(current, above_rows, lax.dynamic_slice_in_dim(scaled, start, RB, 0), lax.dynamic_slice_in_dim(present, start, RB, 0))
        fresh = lax.map(group_update, jnp.arange(N_GRP, dtype=jnp.int32)).reshape((slab_rows,) + blocks.shape[1:])
        return lax.dynamic_update_slice_in_dim(padded_state, fresh, (slab_start + band_reach).astype(jnp.int32), 0)
    for sweep_index in range(ITERS):
        padded_state = lax.fori_loop(0, N_SLAB, slab_update, padded_state)
    return padded_state[band_reach:]
```

```python
import functools

import jax
import jax.numpy as jnp
from jax import lax
from jax.experimental import pallas as pl
from jax.experimental.pallas import tpu as pltpu
from jax.sharding import PartitionSpec as P

AXES = ("slab", "grp")


def idx_a(h, t, s):
    return t * (t + 1) // 2 + s - (h - t)


def idx_b(h, t, s):
    return t * h - t * (t - 1) // 2 + s


def list_a(h):
    return [(t, s) for t in range(h) for s in range(h - t, h + 1)]


def list_b(h):
    return [(t, s) for t in range(h) for s in range(h - t)]


def iotas(n):
    rows = lax.broadcasted_iota(jnp.int32, (n, n), 0)
    cols = lax.broadcasted_iota(jnp.int32, (n, n), 1)
    return rows, cols


def take_diag(block):
    rows, cols = iotas(block.shape[0])
    return jnp.sum(jnp.where(rows == cols, block.astype(jnp.float32), 0.0), axis=0, keepdims=True)


def strict_upper(block):
    rows, cols = iotas(block.shape[0])
    return jnp.where(rows < cols, block.astype(jnp.float32), 0.0).astype(jnp.bfloat16)


def strict_lower(block):
    rows, cols = iotas(block.shape[0])
    return jnp.where(rows > cols, block.astype(jnp.float32), 0.0).astype(jnp.bfloat16)


def diag_kernel(blocks_ref, shift_ref, out_ref):
    for t in range(out_ref.shape[0]):
        out_ref[t : t + 1, :] = shift_ref[t : t + 1, :] + take_diag(blocks_ref[t, 0])


def scale_one(block, is_diag, dv_row, rs_col, cs_row, flag):
    value = block.astype(jnp.float32)
    if is_diag:
        rows, cols = iotas(block.shape[0])
        value = jnp.where(rows == cols, dv_row, value)
    value = value * rs_col * cs_row
    return jnp.where(flag > 0, value, 0.0).astype(jnp.bfloat16)


def scale_own_kernel(h, flags_ref, blocks_ref, dv_ref, sc_ref, sct_ref, a_ref, b_ref, l_ref):
    width = 2 * h + 1
    for t in range(h):
        for k in range(width):
            value = scale_one(
                blocks_ref[t, k],
                k == h,
                dv_ref[h + t : h + t + 1, :],
                sct_ref[:, h + t : h + t + 1],
                sc_ref[t + k : t + k + 1, :],
                flags_ref[t * width + k],
            )
            s = k - h
            if s < 0:
                l_ref[t * h + k] = value
            elif s >= h - t:
                a_ref[idx_a(h, t, s)] = value
            else:
                b_ref[idx_b(h, t, s)] = value


def scale_recv_kernel(h, entries, flags_ref, in_ref, dv_ref, sc_ref, sct_ref, out_ref):
    for n, (t, s) in enumerate(entries):
        out_ref[n] = scale_one(
            in_ref[n],
            s == 0,
            dv_ref[t : t + 1, :],
            sct_ref[:, t : t + 1],
            sc_ref[t + s : t + s + 1, :],
            flags_ref[t * (h + 1) + s],
        )


def upper_kernel(h, flags_ref, ra_ref, sa_ref, sb_ref, a_ref, b_ref, l_ref, oa_ref, ob_ref):
    width = 2 * h + 1

    def own(t, s):
        return a_ref[idx_a(h, t, s)] if s >= h - t else b_ref[idx_b(h, t, s)]

    def above(t, s):
        return own(t, s) if t >= 0 else ra_ref[idx_a(h, t + h, s)]

    @pl.when(flags_ref[h * width] == 0)
    def _():
        oa_ref[...] = a_ref[...]
        ob_ref[...] = b_ref[...]

    @pl.when(flags_ref[h * width] != 0)
    def _():
        for r in range(h):
            for s in range(h + 1):
                in_a = s >= h - r
                o_ref, s_ref = (oa_ref, sa_ref) if in_a else (ob_ref, sb_ref)
                n = idx_a(h, r, s) if in_a else idx_b(h, r, s)

                def block(r=r, s=s, o_ref=o_ref, s_ref=s_ref, n=n):
                    reach = range(1, h - s + 1)
                    diag = own(r, 0)
                    left = [l_ref[r * h + h - m] for m in reach] + [strict_lower(diag)]
                    right = [above(r - m, s + m) for m in reach]
                    right.append(strict_upper(diag) if s == 0 else own(r, s))
                    rest = s_ref[n].astype(jnp.float32) - jnp.dot(
                        jnp.concatenate(left, axis=1),
                        jnp.concatenate(right, axis=0),
                        preferred_element_type=jnp.float32,
                    )
                    if s == 0:
                        rows, cols = iotas(rest.shape[0])
                        rest = jnp.where(rows > cols, rest * (1.0 / take_diag(diag)), rest)
                    o_ref[n] = rest.astype(jnp.bfloat16)

                if s == 0:
                    block()
                else:
                    flag = flags_ref[r * width + h + s]
                    pl.when(flag != 0)(block)

                    @pl.when(flag == 0)
                    def _(o_ref=o_ref, n=n):
                        o_ref[n] = jnp.zeros(o_ref.shape[1:], o_ref.dtype)


def lower_blocks(h, flags_ref, ra_ref, rb_ref, sl_ref, a_ref, b_ref, l_ref, store):
    width = 2 * h + 1

    def above(t, s):
        if t >= 0:
            return a_ref[idx_a(h, t, s)] if s >= h - t else b_ref[idx_b(h, t, s)]
        t = t + h
        return ra_ref[idx_a(h, t, s)] if s >= h - t else rb_ref[idx_b(h, t, s)]

    for r in range(h):
        for k in range(h):
            flag = flags_ref[r * width + k]

            @pl.when(flag != 0)
            def _(r=r, k=k):
                reach = range(h - k, h + 1)
                pivot = above(r - h + k, 0)
                left = [l_ref[r * h + h - m] for m in reach]
                right = [strict_upper(pivot)] + [above(r - m, k - h + m) for m in reach[1:]]
                rest = sl_ref[r * h + k].astype(jnp.float32) - jnp.dot(
                    jnp.concatenate(left, axis=1),
                    jnp.concatenate(right, axis=0),
                    preferred_element_type=jnp.float32,
                )
                store(r, k, (rest * (1.0 / take_diag(pivot))).astype(jnp.bfloat16))

            @pl.when(flag == 0)
            def _(r=r, k=k):
                store(r, k, jnp.zeros(sl_ref.shape[1:], jnp.bfloat16))


def lower_kernel(h, flags_ref, ra_ref, rb_ref, sl_ref, a_ref, b_ref, l_ref, o_ref):
    @pl.when(flags_ref[h * (2 * h + 1)] == 0)
    def _():
        o_ref[...] = l_ref[...]

    @pl.when(flags_ref[h * (2 * h + 1)] != 0)
    def _():
        def store(r, k, value):
            o_ref[r * h + k] = value

        lower_blocks(h, flags_ref, ra_ref, rb_ref, sl_ref, a_ref, b_ref, l_ref, store)


def last_kernel(h, flags_ref, ra_ref, rb_ref, sl_ref, a_ref, b_ref, l_ref, na_ref, nb_ref, o_ref):
    for n, (t, s) in enumerate(list_a(h)):
        o_ref[t, h + s] = na_ref[n]
    for n, (t, s) in enumerate(list_b(h)):
        o_ref[t, h + s] = nb_ref[n]

    @pl.when(flags_ref[h * (2 * h + 1)] == 0)
    def _():
        for t in range(h):
            for k in range(h):
                o_ref[t, k] = l_ref[t * h + k]

    @pl.when(flags_ref[h * (2 * h + 1)] != 0)
    def _():
        def store(r, k, value):
            o_ref[r, k] = value

        lower_blocks(h, flags_ref, ra_ref, rb_ref, sl_ref, a_ref, b_ref, l_ref, store)


def call(body, outs, name, products, smem_first=True):
    specs = [pl.BlockSpec(memory_space=pltpu.SMEM)] if smem_first else []

    def run(*args):
        vmem = [pl.BlockSpec(memory_space=pltpu.VMEM)] * (len(args) - len(specs))
        block = outs[0].shape[-1]
        nbytes = sum(x.size * x.dtype.itemsize for x in list(args) + list(outs))
        return pl.pallas_call(
            body,
            out_shape=outs,
            in_specs=specs + vmem,
            out_specs=[pl.BlockSpec(memory_space=pltpu.VMEM)] * len(outs),
            compiler_params=pltpu.CompilerParams(vmem_limit_bytes=48 * 1024 * 1024),
            cost_estimate=pl.CostEstimate(
                flops=2 * products * block**3, bytes_accessed=nbytes, transcendentals=0
            ),
            name=name,
        )(*args)

    return run


def per_device(blocks, diag_shift, offsets):
    rows, width, size, _ = blocks.shape
    h = (width - 1) // 2
    groups = lax.axis_size("grp")
    devices = lax.axis_size("slab") * groups
    assert rows == h and groups >= 3
    grp = lax.axis_index("grp")
    device = lax.axis_index("slab") * groups + grp
    pairs = [(i, i + 1) for i in range(devices - 1)]
    bf = jnp.bfloat16
    half = h * (h + 1) // 2
    pack = jax.ShapeDtypeStruct((half, size, size), bf)
    lows = jax.ShapeDtypeStruct((h * h, size, size), bf)

    first_pairs = [p for p in pairs if p[1] % groups != 0]
    raw_a = jnp.concatenate([blocks[t, 2 * h - t :] for t in range(h)], 0)
    raw_b = jnp.concatenate([blocks[t, h : 2 * h - t] for t in range(h)], 0)

    own_values = pl.pallas_call(
        diag_kernel,
        grid=(1,),
        in_specs=[
            pl.BlockSpec((rows, 1, size, size), lambda i: (0, h, 0, 0)),
            pl.BlockSpec((rows, size), lambda i: (0, 0)),
        ],
        out_specs=pl.BlockSpec((rows, size), lambda i: (0, 0)),
        out_shape=jax.ShapeDtypeStruct((rows, size), jnp.float32),
        name="diag",
    )(blocks, diag_shift.reshape(rows, size))
    reach_up = jnp.broadcast_to(offsets[:, 1:2].astype(jnp.float32), (rows, 128))
    small = jnp.concatenate([own_values, reach_up], 1)
    before = lax.ppermute(small, AXES, pairs)
    after = lax.ppermute(own_values, AXES, [(j, i) for i, j in pairs])
    halo_a = lax.ppermute(raw_a, AXES, first_pairs)
    halo_b = lax.ppermute(raw_b, AXES, first_pairs)

    widened = jnp.concatenate([before[:, :size], own_values, after], 0)
    positive = widened > 0
    scales = jnp.where(positive, 1.0 / jnp.sqrt(jnp.where(positive, widened, 1.0)), 0.0)
    scales_t = scales.T

    all_rows = rows * devices
    row_ids = device * rows + jnp.arange(rows, dtype=jnp.int32)
    relative = jnp.arange(width, dtype=jnp.int32) - h
    target = row_ids[:, None] + relative[None, :]
    left_side = (relative < 0) & (-relative <= offsets[:, 0:1]) & (target >= 0)
    right_side = (relative > 0) & (relative <= offsets[:, 1:2]) & (target < all_rows)
    present = ((relative == 0) | left_side | right_side).astype(jnp.int32).reshape(-1)
    steps = jnp.arange(h + 1, dtype=jnp.int32)
    before_reach = before[:, size : size + 1].astype(jnp.int32)
    before_target = row_ids[:, None] - rows + steps[None, :]
    before_present = (steps == 0) | ((steps <= before_reach) & (before_target < all_rows))
    before_present = before_present.astype(jnp.int32).reshape(-1)

    sa, sb, sl = call(functools.partial(scale_own_kernel, h), [pack, pack, lows], "scale", 1)(
        present, blocks, widened, scales, scales_t
    )
    (ra,) = call(functools.partial(scale_recv_kernel, h, list_a(h)), [pack], "scale_a", 1)(
        before_present, halo_a, widened, scales, scales_t
    )
    (rb,) = call(functools.partial(scale_recv_kernel, h, list_b(h)), [pack], "scale_b", 1)(
        before_present, halo_b, widened, scales, scales_t
    )

    def flags(active):
        return jnp.concatenate([present, active.astype(jnp.int32).reshape(1)])

    upper = call(functools.partial(upper_kernel, h), [pack, pack], "upper", 30)
    lower = call(functools.partial(lower_kernel, h), [lows], "lower", 20)
    last = call(functools.partial(last_kernel, h), [jax.ShapeDtypeStruct(blocks.shape, bf)], "last", 20)

    on = flags(grp > 0)
    a1, b1 = upper(on, ra, sa, sb, sa, sb, sl)
    second_pairs = [p for p in pairs if p[1] % groups != 1]
    ra1 = lax.ppermute(a1, AXES, second_pairs)
    rb1 = lax.ppermute(b1, AXES, second_pairs)
    (l1,) = lower(on, ra, rb, sl, sa, sb, sl)

    on = flags(grp != 1)
    a2, b2 = upper(on, ra1, sa, sb, a1, b1, l1)
    third_pairs = [p for p in pairs if p[1] % groups < 2]
    ra2 = lax.ppermute(a2, AXES, third_pairs)
    rb2 = lax.ppermute(b2, AXES, third_pairs)
    (l2,) = lower(on, ra1, rb1, sl, a1, b1, l1)

    on = flags(grp < 2)
    a3, b3 = upper(on, ra2, sa, sb, a2, b2, l2)
    (out,) = last(on, ra2, rb2, sl, a2, b2, l2, a3, b3)
    return out


def solution(mesh):
    return jax.shard_map(
        per_device,
        mesh=mesh,
        in_specs=(
            P(AXES, None, None, None),
            P(AXES),
            P(AXES, None),
        ),
        out_specs=P(AXES, None, None, None),
        check_vma=False,
    )
```

```python
import functools

import jax
import jax.numpy as jnp
from jax import lax
from jax.experimental import pallas as pl
from jax.experimental.pallas import tpu as pltpu
from jax.sharding import PartitionSpec as P

AXES = ("slab", "grp")


def idx_a(h, t, s):
    return t * (t + 1) // 2 + s - (h - t)


def idx_b(h, t, s):
    return t * h - t * (t - 1) // 2 + s


def list_a(h):
    return [(t, s) for t in range(h) for s in range(h - t, h + 1)]


def list_b(h):
    return [(t, s) for t in range(h) for s in range(h - t)]


def iotas(n):
    rows = lax.broadcasted_iota(jnp.int32, (n, n), 0)
    cols = lax.broadcasted_iota(jnp.int32, (n, n), 1)
    return rows, cols


def take_diag(block):
    rows, cols = iotas(block.shape[0])
    return jnp.sum(jnp.where(rows == cols, block.astype(jnp.float32), 0.0), axis=0, keepdims=True)


def strict_upper(block):
    rows, cols = iotas(block.shape[0])
    return jnp.where(rows < cols, block.astype(jnp.float32), 0.0).astype(jnp.bfloat16)


def strict_lower(block):
    rows, cols = iotas(block.shape[0])
    return jnp.where(rows > cols, block.astype(jnp.float32), 0.0).astype(jnp.bfloat16)


def pack_kernel(h, shift_ref, *refs):
    columns = refs[: h + 1]
    values_ref, a_ref, b_ref = refs[h + 1 :]
    size = a_ref.shape[1]
    for t in range(h):
        shift = shift_ref[t * size : (t + 1) * size].reshape(1, size)
        values_ref[t : t + 1, :] = shift + take_diag(columns[0][t, 0])
    for n, (t, s) in enumerate(list_a(h)):
        a_ref[n] = columns[s][t, 0]
    for n, (t, s) in enumerate(list_b(h)):
        b_ref[n] = columns[s][t, 0]


def scale_one(block, is_diag, dv_row, rs_col, cs_row, flag):
    value = block.astype(jnp.float32)
    if is_diag:
        rows, cols = iotas(block.shape[0])
        value = jnp.where(rows == cols, dv_row, value)
    value = value * rs_col * cs_row
    return jnp.where(flag > 0, value, 0.0).astype(jnp.bfloat16)


def scale_own_kernel(h, flags_ref, blocks_ref, dv_ref, sc_ref, sct_ref, a_ref, b_ref, l_ref):
    width = 2 * h + 1
    for t in range(h):
        for k in range(width):
            value = scale_one(
                blocks_ref[t, k],
                k == h,
                dv_ref[h + t : h + t + 1, :],
                sct_ref[:, h + t : h + t + 1],
                sc_ref[t + k : t + k + 1, :],
                flags_ref[t * width + k],
            )
            s = k - h
            if s < 0:
                l_ref[t * h + k] = value
            elif s >= h - t:
                a_ref[idx_a(h, t, s)] = value
            else:
                b_ref[idx_b(h, t, s)] = value


def scale_recv_kernel(h, entries, flags_ref, in_ref, dv_ref, sc_ref, sct_ref, out_ref):
    for n, (t, s) in enumerate(entries):
        out_ref[n] = scale_one(
            in_ref[n],
            s == 0,
            dv_ref[t : t + 1, :],
            sct_ref[:, t : t + 1],
            sc_ref[t + s : t + s + 1, :],
            flags_ref[t * (h + 1) + s],
        )


def upper_kernel(h, flags_ref, ra_ref, sa_ref, sb_ref, a_ref, b_ref, l_ref, oa_ref, ob_ref):
    width = 2 * h + 1

    def own(t, s):
        return a_ref[idx_a(h, t, s)] if s >= h - t else b_ref[idx_b(h, t, s)]

    def above(t, s):
        return own(t, s) if t >= 0 else ra_ref[idx_a(h, t + h, s)]

    @pl.when(flags_ref[h * width] == 0)
    def _():
        oa_ref[...] = a_ref[...]
        ob_ref[...] = b_ref[...]

    @pl.when(flags_ref[h * width] != 0)
    def _():
        for r in range(h):
            for s in range(h + 1):
                in_a = s >= h - r
                o_ref, s_ref = (oa_ref, sa_ref) if in_a else (ob_ref, sb_ref)
                n = idx_a(h, r, s) if in_a else idx_b(h, r, s)

                def block(r=r, s=s, o_ref=o_ref, s_ref=s_ref, n=n):
                    reach = range(1, h - s + 1)
                    diag = own(r, 0)
                    left = [l_ref[r * h + h - m] for m in reach] + [strict_lower(diag)]
                    right = [above(r - m, s + m) for m in reach]
                    right.append(strict_upper(diag) if s == 0 else own(r, s))
                    rest = s_ref[n].astype(jnp.float32) - jnp.dot(
                        jnp.concatenate(left, axis=1),
                        jnp.concatenate(right, axis=0),
                        preferred_element_type=jnp.float32,
                    )
                    if s == 0:
                        rows, cols = iotas(rest.shape[0])
                        rest = jnp.where(rows > cols, rest * (1.0 / take_diag(diag)), rest)
                    o_ref[n] = rest.astype(jnp.bfloat16)

                if s == 0:
                    block()
                else:
                    flag = flags_ref[r * width + h + s]
                    pl.when(flag != 0)(block)

                    @pl.when(flag == 0)
                    def _(o_ref=o_ref, n=n):
                        o_ref[n] = jnp.zeros(o_ref.shape[1:], o_ref.dtype)


def lower_blocks(h, flags_ref, ra_ref, rb_ref, sl_ref, a_ref, b_ref, l_ref, store, wanted):
    width = 2 * h + 1

    def above(t, s):
        if t >= 0:
            return a_ref[idx_a(h, t, s)] if s >= h - t else b_ref[idx_b(h, t, s)]
        t = t + h
        return ra_ref[idx_a(h, t, s)] if s >= h - t else rb_ref[idx_b(h, t, s)]

    for r in range(h):
        for k in range(h):
            if not wanted(r, k):
                continue
            flag = flags_ref[r * width + k]

            @pl.when(flag != 0)
            def _(r=r, k=k):
                reach = range(h - k, h + 1)
                pivot = above(r - h + k, 0)
                left = [l_ref[r * h + h - m] for m in reach]
                right = [strict_upper(pivot)] + [above(r - m, k - h + m) for m in reach[1:]]
                rest = sl_ref[r * h + k].astype(jnp.float32) - jnp.dot(
                    jnp.concatenate(left, axis=1),
                    jnp.concatenate(right, axis=0),
                    preferred_element_type=jnp.float32,
                )
                store(r, k, (rest * (1.0 / take_diag(pivot))).astype(jnp.bfloat16))

            @pl.when(flag == 0)
            def _(r=r, k=k):
                store(r, k, jnp.zeros(sl_ref.shape[1:], jnp.bfloat16))


def lower_kernel(h, flags_ref, ra_ref, rb_ref, sl_ref, a_ref, b_ref, l_ref, o_ref):
    @pl.when(flags_ref[h * (2 * h + 1)] == 0)
    def _():
        o_ref[...] = l_ref[...]

    @pl.when(flags_ref[h * (2 * h + 1)] != 0)
    def _():
        def store(r, k, value):
            o_ref[r * h + k] = value

        lower_blocks(
            h, flags_ref, ra_ref, rb_ref, sl_ref, a_ref, b_ref, l_ref, store, lambda r, k: True
        )


def middle_kernel(h, flags_ref, ra_ref, sl_ref, a_ref, b_ref, l_ref, na_ref, nb_ref, o_ref):
    for n, (t, s) in enumerate(list_a(h)):
        o_ref[t, h + s] = na_ref[n]
    for n, (t, s) in enumerate(list_b(h)):
        o_ref[t, h + s] = nb_ref[n]
    idle = flags_ref[h * (2 * h + 1)] == 0

    @pl.when(idle)
    def _():
        for t in range(h):
            for k in range(h):
                o_ref[t, k] = l_ref[t * h + k]

    @pl.when(jnp.logical_not(idle))
    def _():
        def store(r, k, value):
            o_ref[r, k] = value

        def wanted(r, k):
            return k >= h - r

        for t in range(h):
            for k in range(h - t):
                o_ref[t, k] = jnp.zeros(o_ref.shape[2:], o_ref.dtype)
        lower_blocks(
            h, flags_ref, ra_ref, None, sl_ref, a_ref, b_ref, l_ref, store, wanted
        )


def last_kernel(h, flags_ref, rb_ref, sl_ref, l_ref, out_in_ref, o_ref, buf_ref, sems):
    del out_in_ref

    @pl.when(flags_ref[h * (2 * h + 1)] != 0)
    def _():
        entries = [(r, k) for r in range(h) for k in range(h - r)]

        def copy(n):
            r, k = entries[n]
            return pltpu.make_async_copy(buf_ref.at[n], o_ref.at[r, k], sems.at[n])

        def store(r, k, value):
            buf_ref[entries.index((r, k))] = value

        for n, entry in enumerate(entries):
            lower_blocks(
                h, flags_ref, None, rb_ref, sl_ref, None, None, l_ref, store,
                lambda r, k, entry=entry: (r, k) == entry,
            )
            copy(n).start()
        for n in range(len(entries)):
            copy(n).wait()


def call(body, outs, name, products, smem_first=True):
    specs = [pl.BlockSpec(memory_space=pltpu.SMEM)] if smem_first else []

    def run(*args):
        vmem = [pl.BlockSpec(memory_space=pltpu.VMEM)] * (len(args) - len(specs))
        block = outs[0].shape[-1]
        nbytes = sum(x.size * x.dtype.itemsize for x in list(args) + list(outs))
        return pl.pallas_call(
            body,
            out_shape=outs,
            in_specs=specs + vmem,
            out_specs=[pl.BlockSpec(memory_space=pltpu.VMEM)] * len(outs),
            compiler_params=pltpu.CompilerParams(vmem_limit_bytes=48 * 1024 * 1024),
            cost_estimate=pl.CostEstimate(
                flops=2 * products * block**3, bytes_accessed=nbytes, transcendentals=0
            ),
            name=name,
        )(*args)

    return run


def per_device(blocks, diag_shift, offsets):
    rows, width, size, _ = blocks.shape
    h = (width - 1) // 2
    groups = lax.axis_size("grp")
    devices = lax.axis_size("slab") * groups
    assert rows == h and groups >= 3
    grp = lax.axis_index("grp")
    device = lax.axis_index("slab") * groups + grp
    pairs = [(i, i + 1) for i in range(devices - 1)]
    bf = jnp.bfloat16
    half = h * (h + 1) // 2
    pack = jax.ShapeDtypeStruct((half, size, size), bf)
    lows = jax.ShapeDtypeStruct((h * h, size, size), bf)

    first_pairs = [p for p in pairs if p[1] % groups != 0]
    own_values, raw_a, raw_b = pl.pallas_call(
        functools.partial(pack_kernel, h),
        grid=(1,),
        in_specs=[pl.BlockSpec((rows * size,), lambda i: (0,))]
        + [
            pl.BlockSpec((rows, 1, size, size), functools.partial(lambda k, i: (0, k, 0, 0), h + s))
            for s in range(h + 1)
        ],
        out_specs=[
            pl.BlockSpec((rows, size), lambda i: (0, 0)),
            pl.BlockSpec((half, size, size), lambda i: (0, 0, 0)),
            pl.BlockSpec((half, size, size), lambda i: (0, 0, 0)),
        ],
        out_shape=[jax.ShapeDtypeStruct((rows, size), jnp.float32), pack, pack],
        name="pack",
    )(diag_shift, *([blocks] * (h + 1)))
    reach_up = jnp.broadcast_to(offsets[:, 1:2].astype(jnp.float32), (rows, 128))
    small = jnp.concatenate([own_values, reach_up], 1)
    before = lax.ppermute(small, AXES, pairs)
    after = lax.ppermute(own_values, AXES, [(j, i) for i, j in pairs])
    halo_a = lax.ppermute(raw_a, AXES, first_pairs)
    halo_b = lax.ppermute(raw_b, AXES, first_pairs)

    widened = jnp.concatenate([before[:, :size], own_values, after], 0)
    positive = widened > 0
    scales = jnp.where(positive, 1.0 / jnp.sqrt(jnp.where(positive, widened, 1.0)), 0.0)
    scales_t = scales.T

    all_rows = rows * devices
    row_ids = device * rows + jnp.arange(rows, dtype=jnp.int32)
    relative = jnp.arange(width, dtype=jnp.int32) - h
    target = row_ids[:, None] + relative[None, :]
    left_side = (relative < 0) & (-relative <= offsets[:, 0:1]) & (target >= 0)
    right_side = (relative > 0) & (relative <= offsets[:, 1:2]) & (target < all_rows)
    present = ((relative == 0) | left_side | right_side).astype(jnp.int32).reshape(-1)
    steps = jnp.arange(h + 1, dtype=jnp.int32)
    before_reach = before[:, size : size + 1].astype(jnp.int32)
    before_target = row_ids[:, None] - rows + steps[None, :]
    before_present = (steps == 0) | ((steps <= before_reach) & (before_target < all_rows))
    before_present = before_present.astype(jnp.int32).reshape(-1)

    sa, sb, sl = call(functools.partial(scale_own_kernel, h), [pack, pack, lows], "scale", 1)(
        present, blocks, widened, scales, scales_t
    )
    (ra,) = call(functools.partial(scale_recv_kernel, h, list_a(h)), [pack], "scale_a", 1)(
        before_present, halo_a, widened, scales, scales_t
    )
    (rb,) = call(functools.partial(scale_recv_kernel, h, list_b(h)), [pack], "scale_b", 1)(
        before_present, halo_b, widened, scales, scales_t
    )

    def flags(active):
        return jnp.concatenate([present, active.astype(jnp.int32).reshape(1)])

    upper = call(functools.partial(upper_kernel, h), [pack, pack], "upper", 30)
    lower = call(functools.partial(lower_kernel, h), [lows], "lower", 20)
    full = jax.ShapeDtypeStruct(blocks.shape, bf)
    middle = call(functools.partial(middle_kernel, h), [full], "middle", 10)
    vmem = pl.BlockSpec(memory_space=pltpu.VMEM)
    anywhere = pl.BlockSpec(memory_space=pl.ANY)
    last = pl.pallas_call(
        functools.partial(last_kernel, h),
        out_shape=full,
        in_specs=[pl.BlockSpec(memory_space=pltpu.SMEM), vmem, vmem, vmem, anywhere],
        out_specs=anywhere,
        scratch_shapes=[pltpu.VMEM((half, size, size), bf), pltpu.SemaphoreType.DMA((half,))],
        input_output_aliases={4: 0},
        compiler_params=pltpu.CompilerParams(vmem_limit_bytes=32 * 1024 * 1024),
        cost_estimate=pl.CostEstimate(
            flops=20 * size**3, bytes_accessed=blocks.size, transcendentals=0
        ),
        name="last",
    )

    on = flags(grp > 0)
    a1, b1 = upper(on, ra, sa, sb, sa, sb, sl)
    second_pairs = [p for p in pairs if p[1] % groups != 1]
    ra1 = lax.ppermute(a1, AXES, second_pairs)
    rb1 = lax.ppermute(b1, AXES, second_pairs)
    (l1,) = lower(on, ra, rb, sl, sa, sb, sl)

    on = flags(grp != 1)
    a2, b2 = upper(on, ra1, sa, sb, a1, b1, l1)
    third_pairs = [p for p in pairs if p[1] % groups < 2]
    ra2 = lax.ppermute(a2, AXES, third_pairs)
    rb2 = lax.ppermute(b2, AXES, third_pairs)
    (l2,) = lower(on, ra1, rb1, sl, a1, b1, l1)

    on = flags(grp < 2)
    a3, b3 = upper(on, ra2, sa, sb, a2, b2, l2)
    (out,) = middle(on, ra2, sl, a2, b2, l2, a3, b3)
    out = last(on, rb2, sl, l2, out)
    return out


def solution(mesh):
    return jax.shard_map(
        per_device,
        mesh=mesh,
        in_specs=(
            P(AXES, None, None, None),
            P(AXES),
            P(AXES, None),
        ),
        out_specs=P(AXES, None, None, None),
        check_vma=False,
    )
```

```python
import functools

import jax
import jax.numpy as jnp
from jax import lax
from jax.experimental import pallas as pl
from jax.experimental.pallas import tpu as pltpu
from jax.sharding import PartitionSpec as P


AXES = ("slab", "grp")


def idx_a(h, t, s):
    return t * (t + 1) // 2 + s - (h - t)


def idx_b(h, t, s):
    return t * h - t * (t - 1) // 2 + s


def list_a(h):
    return [(t, s) for t in range(h) for s in range(h - t, h + 1)]


def list_b(h):
    return [(t, s) for t in range(h) for s in range(h - t)]


def iotas(n):
    rows = lax.broadcasted_iota(jnp.int32, (n, n), 0)
    cols = lax.broadcasted_iota(jnp.int32, (n, n), 1)
    return rows, cols


def take_diag(block):
    rows, cols = iotas(block.shape[0])
    return jnp.sum(jnp.where(rows == cols, block.astype(jnp.float32), 0.0), axis=0, keepdims=True)


def strict_upper(block):
    rows, cols = iotas(block.shape[0])
    return jnp.where(rows < cols, block.astype(jnp.float32), 0.0).astype(jnp.bfloat16)


def strict_lower(block):
    rows, cols = iotas(block.shape[0])
    return jnp.where(rows > cols, block.astype(jnp.float32), 0.0).astype(jnp.bfloat16)


def pack_kernel(h, shift_ref, *refs):
    columns = refs[: h + 1]
    values_ref, a_ref, b_ref = refs[h + 1 :]
    size = a_ref.shape[1]
    for t in range(h):
        shift = shift_ref[t * size : (t + 1) * size].reshape(1, size)
        values_ref[t : t + 1, :] = shift + take_diag(columns[0][t, 0])
    for n, (t, s) in enumerate(list_a(h)):
        a_ref[n] = columns[s][t, 0]
    for n, (t, s) in enumerate(list_b(h)):
        b_ref[n] = columns[s][t, 0]


def scale_one(block, is_diag, dv_row, rs_col, cs_row, flag):
    value = block.astype(jnp.float32)
    if is_diag:
        rows, cols = iotas(block.shape[0])
        value = jnp.where(rows == cols, dv_row, value)
    value = value * rs_col * cs_row
    return jnp.where(flag > 0, value, 0.0).astype(jnp.bfloat16)


def scale_own_kernel(h, flags_ref, blocks_ref, dv_ref, sc_ref, sct_ref, a_ref, b_ref, l_ref):
    width = 2 * h + 1
    for t in range(h):
        for k in range(width):
            value = scale_one(
                blocks_ref[t, k],
                k == h,
                dv_ref[h + t : h + t + 1, :],
                sct_ref[:, h + t : h + t + 1],
                sc_ref[t + k : t + k + 1, :],
                flags_ref[t * width + k],
            )
            s = k - h
            if s < 0:
                l_ref[t * h + k] = value
            elif s >= h - t:
                a_ref[idx_a(h, t, s)] = value
            else:
                b_ref[idx_b(h, t, s)] = value


def scale_recv_kernel(h, entries, flags_ref, in_ref, dv_ref, sc_ref, sct_ref, out_ref):
    for n, (t, s) in enumerate(entries):
        out_ref[n] = scale_one(
            in_ref[n],
            s == 0,
            dv_ref[t : t + 1, :],
            sct_ref[:, t : t + 1],
            sc_ref[t + s : t + s + 1, :],
            flags_ref[t * (h + 1) + s],
        )


def upper_blocks(h, flags_ref, ra_ref, sa_ref, sb_ref, a_ref, b_ref, l_ref, store):
    width = 2 * h + 1

    def own(t, s):
        return a_ref[idx_a(h, t, s)] if s >= h - t else b_ref[idx_b(h, t, s)]

    def above(t, s):
        return own(t, s) if t >= 0 else ra_ref[idx_a(h, t + h, s)]

    for r in range(h):
        for s in range(h + 1):
            in_a = s >= h - r
            s_ref = sa_ref if in_a else sb_ref
            n = idx_a(h, r, s) if in_a else idx_b(h, r, s)

            def block(r=r, s=s, s_ref=s_ref, n=n):
                reach = range(1, h - s + 1)
                diag = own(r, 0)
                left = [l_ref[r * h + h - m] for m in reach] + [strict_lower(diag)]
                right = [above(r - m, s + m) for m in reach]
                right.append(strict_upper(diag) if s == 0 else own(r, s))
                rest = s_ref[n].astype(jnp.float32) - jnp.dot(
                    jnp.concatenate(left, axis=1),
                    jnp.concatenate(right, axis=0),
                    preferred_element_type=jnp.float32,
                )
                if s == 0:
                    rows, cols = iotas(rest.shape[0])
                    rest = jnp.where(rows > cols, rest * (1.0 / take_diag(diag)), rest)
                store(r, s, rest.astype(jnp.bfloat16))

            if s == 0:
                block()
            else:
                flag = flags_ref[r * width + h + s]
                pl.when(flag != 0)(block)

                @pl.when(flag == 0)
                def _(r=r, s=s):
                    store(r, s, jnp.zeros(sa_ref.shape[1:], jnp.bfloat16))


def upper_kernel(h, flags_ref, ra_ref, sa_ref, sb_ref, a_ref, b_ref, l_ref, oa_ref, ob_ref):
    idle = flags_ref[h * (2 * h + 1)] == 0

    @pl.when(idle)
    def _():
        oa_ref[...] = a_ref[...]
        ob_ref[...] = b_ref[...]

    @pl.when(jnp.logical_not(idle))
    def _():
        def store(r, s, value):
            if s >= h - r:
                oa_ref[idx_a(h, r, s)] = value
            else:
                ob_ref[idx_b(h, r, s)] = value

        upper_blocks(h, flags_ref, ra_ref, sa_ref, sb_ref, a_ref, b_ref, l_ref, store)


def lower_blocks(h, flags_ref, ra_ref, rb_ref, sl_ref, a_ref, b_ref, l_ref, store, wanted):
    width = 2 * h + 1

    def above(t, s):
        if t >= 0:
            return a_ref[idx_a(h, t, s)] if s >= h - t else b_ref[idx_b(h, t, s)]
        t = t + h
        return ra_ref[idx_a(h, t, s)] if s >= h - t else rb_ref[idx_b(h, t, s)]

    for r in range(h):
        for k in range(h):
            if not wanted(r, k):
                continue
            flag = flags_ref[r * width + k]

            @pl.when(flag != 0)
            def _(r=r, k=k):
                reach = range(h - k, h + 1)
                pivot = above(r - h + k, 0)
                left = [l_ref[r * h + h - m] for m in reach]
                right = [strict_upper(pivot)] + [above(r - m, k - h + m) for m in reach[1:]]
                rest = sl_ref[r * h + k].astype(jnp.float32) - jnp.dot(
                    jnp.concatenate(left, axis=1),
                    jnp.concatenate(right, axis=0),
                    preferred_element_type=jnp.float32,
                )
                store(r, k, (rest * (1.0 / take_diag(pivot))).astype(jnp.bfloat16))

            @pl.when(flag == 0)
            def _(r=r, k=k):
                store(r, k, jnp.zeros(sl_ref.shape[1:], jnp.bfloat16))


def lower_kernel(h, flags_ref, ra_ref, rb_ref, sl_ref, a_ref, b_ref, l_ref, o_ref):
    @pl.when(flags_ref[h * (2 * h + 1)] == 0)
    def _():
        o_ref[...] = l_ref[...]

    @pl.when(flags_ref[h * (2 * h + 1)] != 0)
    def _():
        def store(r, k, value):
            o_ref[r * h + k] = value

        lower_blocks(
            h, flags_ref, ra_ref, rb_ref, sl_ref, a_ref, b_ref, l_ref, store, lambda r, k: True
        )


def middle_kernel(h, flags_ref, ra_ref, sa_ref, sb_ref, sl_ref, a_ref, b_ref, l_ref, o_ref):
    idle = flags_ref[h * (2 * h + 1)] == 0

    @pl.when(idle)
    def _():
        for n, (t, s) in enumerate(list_a(h)):
            o_ref[t, h + s] = a_ref[n]
        for n, (t, s) in enumerate(list_b(h)):
            o_ref[t, h + s] = b_ref[n]
        for t in range(h):
            for k in range(h):
                o_ref[t, k] = l_ref[t * h + k]

    @pl.when(jnp.logical_not(idle))
    def _():
        def store_upper(r, s, value):
            o_ref[r, h + s] = value

        def store(r, k, value):
            o_ref[r, k] = value

        def wanted(r, k):
            return k >= h - r

        for t in range(h):
            for k in range(h - t):
                o_ref[t, k] = jnp.zeros(o_ref.shape[2:], o_ref.dtype)
        upper_blocks(h, flags_ref, ra_ref, sa_ref, sb_ref, a_ref, b_ref, l_ref, store_upper)
        lower_blocks(
            h, flags_ref, ra_ref, None, sl_ref, a_ref, b_ref, l_ref, store, wanted
        )


def last_kernel(h, flags_ref, rb_ref, sl_ref, l_ref, out_in_ref, o_ref, buf_ref, sems):
    del out_in_ref

    @pl.when(flags_ref[h * (2 * h + 1)] != 0)
    def _():
        entries = [(r, k) for r in range(h) for k in range(h - r)]

        def copy(n):
            r, k = entries[n]
            return pltpu.make_async_copy(buf_ref.at[n], o_ref.at[r, k], sems.at[n])

        def store(r, k, value):
            buf_ref[entries.index((r, k))] = value

        for n, entry in enumerate(entries):
            lower_blocks(
                h, flags_ref, None, rb_ref, sl_ref, None, None, l_ref, store,
                lambda r, k, entry=entry: (r, k) == entry,
            )
            copy(n).start()
        for n in range(len(entries)):
            copy(n).wait()


def call(body, outs, products, smem_first=True):
    specs = [pl.BlockSpec(memory_space=pltpu.SMEM)] if smem_first else []

    def run(*args):
        vmem = [pl.BlockSpec(memory_space=pltpu.VMEM)] * (len(args) - len(specs))
        block = outs[0].shape[-1]
        nbytes = sum(x.size * x.dtype.itemsize for x in list(args) + list(outs))
        return pl.pallas_call(
            body,
            out_shape=outs,
            in_specs=specs + vmem,
            out_specs=[pl.BlockSpec(memory_space=pltpu.VMEM)] * len(outs),
            compiler_params=pltpu.CompilerParams(vmem_limit_bytes=48 * 1024 * 1024),
            cost_estimate=pl.CostEstimate(
                flops=2 * products * block**3, bytes_accessed=nbytes, transcendentals=0
            ),
        )(*args)

    return run


def per_device(blocks, diag_shift, offsets):
    rows, width, size, _ = blocks.shape
    h = (width - 1) // 2
    groups = lax.axis_size("grp")
    devices = lax.axis_size("slab") * groups
    assert rows == h and groups >= 3
    grp = lax.axis_index("grp")
    device = lax.axis_index("slab") * groups + grp
    pairs = [(i, i + 1) for i in range(devices - 1)]
    bf = jnp.bfloat16
    half = h * (h + 1) // 2
    pack = jax.ShapeDtypeStruct((half, size, size), bf)
    lows = jax.ShapeDtypeStruct((h * h, size, size), bf)

    first_pairs = [p for p in pairs if p[1] % groups != 0]
    own_values, raw_a, raw_b = pl.pallas_call(
        functools.partial(pack_kernel, h),
        grid=(1,),
        in_specs=[pl.BlockSpec((rows * size,), lambda i: (0,))]
        + [
            pl.BlockSpec((rows, 1, size, size), functools.partial(lambda k, i: (0, k, 0, 0), h + s))
            for s in range(h + 1)
        ],
        out_specs=[
            pl.BlockSpec((rows, size), lambda i: (0, 0)),
            pl.BlockSpec((half, size, size), lambda i: (0, 0, 0)),
            pl.BlockSpec((half, size, size), lambda i: (0, 0, 0)),
        ],
        out_shape=[jax.ShapeDtypeStruct((rows, size), jnp.float32), pack, pack],
        name="pack",
    )(diag_shift, *([blocks] * (h + 1)))
    reach_up = jnp.broadcast_to(offsets[:, 1:2].astype(jnp.float32), (rows, 128))
    small = jnp.concatenate([own_values, reach_up], 1)
    before = lax.ppermute(small, AXES, pairs)
    halo_a = lax.ppermute(raw_a, AXES, first_pairs)
    after = lax.ppermute(own_values, AXES, [(j, i) for i, j in pairs])
    halo_b = lax.ppermute(raw_b, AXES, first_pairs)

    widened = jnp.concatenate([before[:, :size], own_values, after], 0)
    positive = widened > 0
    scales = jnp.where(positive, 1.0 / jnp.sqrt(jnp.where(positive, widened, 1.0)), 0.0)
    scales_t = scales.T

    all_rows = rows * devices
    row_ids = device * rows + jnp.arange(rows, dtype=jnp.int32)
    relative = jnp.arange(width, dtype=jnp.int32) - h
    target = row_ids[:, None] + relative[None, :]
    left_side = (relative < 0) & (-relative <= offsets[:, 0:1]) & (target >= 0)
    right_side = (relative > 0) & (relative <= offsets[:, 1:2]) & (target < all_rows)
    present = ((relative == 0) | left_side | right_side).astype(jnp.int32).reshape(-1)
    steps = jnp.arange(h + 1, dtype=jnp.int32)
    before_reach = before[:, size : size + 1].astype(jnp.int32)
    before_target = row_ids[:, None] - rows + steps[None, :]
    before_present = (steps == 0) | ((steps <= before_reach) & (before_target < all_rows))
    before_present = before_present.astype(jnp.int32).reshape(-1)

    sa, sb, sl = call(functools.partial(scale_own_kernel, h), [pack, pack, lows], 1)(
        present, blocks, widened, scales, scales_t
    )
    (ra,) = call(functools.partial(scale_recv_kernel, h, list_a(h)), [pack], 1)(
        before_present, halo_a, widened, scales, scales_t
    )
    (rb,) = call(functools.partial(scale_recv_kernel, h, list_b(h)), [pack], 1)(
        before_present, halo_b, widened, scales, scales_t
    )

    def flags(active):
        return jnp.concatenate([present, active.astype(jnp.int32).reshape(1)])

    upper = call(functools.partial(upper_kernel, h), [pack, pack], 30)
    lower = call(functools.partial(lower_kernel, h), [lows], 20)
    full = jax.ShapeDtypeStruct(blocks.shape, bf)
    middle = call(functools.partial(middle_kernel, h), [full], 50)
    vmem = pl.BlockSpec(memory_space=pltpu.VMEM)
    anywhere = pl.BlockSpec(memory_space=pl.ANY)
    last = pl.pallas_call(
        functools.partial(last_kernel, h),
        out_shape=full,
        in_specs=[pl.BlockSpec(memory_space=pltpu.SMEM), vmem, vmem, vmem, anywhere],
        out_specs=anywhere,
        scratch_shapes=[pltpu.VMEM((half, size, size), bf), pltpu.SemaphoreType.DMA((half,))],
        input_output_aliases={4: 0},
        compiler_params=pltpu.CompilerParams(vmem_limit_bytes=32 * 1024 * 1024),
        cost_estimate=pl.CostEstimate(
            flops=20 * size**3, bytes_accessed=blocks.size, transcendentals=0
        ),
        name="last",
    )

    on = flags(grp > 0)
    a1, b1 = upper(on, ra, sa, sb, sa, sb, sl)
    second_pairs = [p for p in pairs if p[1] % groups != 1]
    ra1 = lax.ppermute(a1, AXES, second_pairs)
    rb1 = lax.ppermute(b1, AXES, second_pairs)
    (l1,) = lower(on, ra, rb, sl, sa, sb, sl)

    on = flags(grp != 1)
    a2, b2 = upper(on, ra1, sa, sb, a1, b1, l1)
    third_pairs = [p for p in pairs if p[1] % groups < 2]
    ra2 = lax.ppermute(a2, AXES, third_pairs)
    rb2 = lax.ppermute(b2, AXES, third_pairs)
    (l2,) = lower(on, ra1, rb1, sl, a1, b1, l1)

    on = flags(grp < 2)
    (out,) = middle(on, ra2, sa, sb, sl, a2, b2, l2)
    out = last(on, rb2, sl, l2, out)
    return out


def solution(mesh):
    return jax.shard_map(
        per_device,
        mesh=mesh,
        in_specs=(
            P(AXES, None, None, None),
            P(AXES),
            P(AXES, None),
        ),
        out_specs=P(AXES, None, None, None),
        check_vma=False,
    )
```

```python
import functools

import jax
import jax.numpy as jnp
from jax import lax
from jax.experimental import pallas as pl
from jax.experimental.pallas import tpu as pltpu
from jax.sharding import PartitionSpec as P

AXES = ("slab", "grp")


def idx_a(h, t, s):
    return t * (t + 1) // 2 + s - (h - t)


def idx_b(h, t, s):
    return t * h - t * (t - 1) // 2 + s


def list_a(h):
    return [(t, s) for t in range(h) for s in range(h - t, h + 1)]


def list_b(h):
    return [(t, s) for t in range(h) for s in range(h - t)]


def iotas(n):
    rows = lax.broadcasted_iota(jnp.int32, (n, n), 0)
    cols = lax.broadcasted_iota(jnp.int32, (n, n), 1)
    return rows, cols


def take_diag(block):
    rows, cols = iotas(block.shape[0])
    return jnp.sum(jnp.where(rows == cols, block.astype(jnp.float32), 0.0), axis=0, keepdims=True)


def strict_upper(block):
    rows, cols = iotas(block.shape[0])
    return jnp.where(rows < cols, block.astype(jnp.float32), 0.0).astype(jnp.bfloat16)


def strict_lower(block):
    rows, cols = iotas(block.shape[0])
    return jnp.where(rows > cols, block.astype(jnp.float32), 0.0).astype(jnp.bfloat16)


def pack_kernel(h, shift_ref, *refs):
    columns = refs[: h + 1]
    values_ref, a_ref, b_ref = refs[h + 1 :]
    size = a_ref.shape[1]
    for t in range(h):
        shift = shift_ref[t * size : (t + 1) * size].reshape(1, size)
        values_ref[t : t + 1, :] = shift + take_diag(columns[0][t, 0])
    for n, (t, s) in enumerate(list_a(h)):
        a_ref[n] = columns[s][t, 0]
    for n, (t, s) in enumerate(list_b(h)):
        b_ref[n] = columns[s][t, 0]


def scale_one(block, is_diag, dv_row, rs_col, cs_row, flag):
    value = block.astype(jnp.float32)
    if is_diag:
        rows, cols = iotas(block.shape[0])
        value = jnp.where(rows == cols, dv_row, value)
    value = value * rs_col * cs_row
    return jnp.where(flag > 0, value, 0.0).astype(jnp.bfloat16)


def scale_own_kernel(h, flags_ref, blocks_ref, dv_ref, sc_ref, sct_ref, a_ref, b_ref, l_ref):
    width = 2 * h + 1
    for t in range(h):
        for k in range(width):
            value = scale_one(
                blocks_ref[t, k],
                k == h,
                dv_ref[h + t : h + t + 1, :],
                sct_ref[:, h + t : h + t + 1],
                sc_ref[t + k : t + k + 1, :],
                flags_ref[t * width + k],
            )
            s = k - h
            if s < 0:
                l_ref[t * h + k] = value
            elif s >= h - t:
                a_ref[idx_a(h, t, s)] = value
            else:
                b_ref[idx_b(h, t, s)] = value


def scale_recv_kernel(h, entries, flags_ref, in_ref, dv_ref, sc_ref, sct_ref, out_ref):
    for n, (t, s) in enumerate(entries):
        out_ref[n] = scale_one(
            in_ref[n],
            s == 0,
            dv_ref[t : t + 1, :],
            sct_ref[:, t : t + 1],
            sc_ref[t + s : t + s + 1, :],
            flags_ref[t * (h + 1) + s],
        )


def upper_blocks(h, flags_ref, ra_ref, sa_ref, sb_ref, a_ref, b_ref, l_ref, store):
    width = 2 * h + 1

    def own(t, s):
        return a_ref[idx_a(h, t, s)] if s >= h - t else b_ref[idx_b(h, t, s)]

    def above(t, s):
        return own(t, s) if t >= 0 else ra_ref[idx_a(h, t + h, s)]

    for r in range(h):
        for s in range(h + 1):
            in_a = s >= h - r
            s_ref = sa_ref if in_a else sb_ref
            n = idx_a(h, r, s) if in_a else idx_b(h, r, s)

            def block(r=r, s=s, s_ref=s_ref, n=n):
                reach = range(1, h - s + 1)
                diag = own(r, 0)
                left = [l_ref[r * h + h - m] for m in reach] + [strict_lower(diag)]
                right = [above(r - m, s + m) for m in reach]
                right.append(strict_upper(diag) if s == 0 else own(r, s))
                rest = s_ref[n].astype(jnp.float32) - jnp.dot(
                    jnp.concatenate(left, axis=1),
                    jnp.concatenate(right, axis=0),
                    preferred_element_type=jnp.float32,
                )
                if s == 0:
                    rows, cols = iotas(rest.shape[0])
                    rest = jnp.where(rows > cols, rest * (1.0 / take_diag(diag)), rest)
                store(r, s, rest.astype(jnp.bfloat16))

            if s == 0:
                block()
            else:
                flag = flags_ref[r * width + h + s]
                pl.when(flag != 0)(block)

                @pl.when(flag == 0)
                def _(r=r, s=s):
                    store(r, s, jnp.zeros(sa_ref.shape[1:], jnp.bfloat16))


def upper_kernel(h, flags_ref, ra_ref, sa_ref, sb_ref, a_ref, b_ref, l_ref, oa_ref, ob_ref):
    idle = flags_ref[h * (2 * h + 1)] == 0

    @pl.when(idle)
    def _():
        oa_ref[...] = a_ref[...]
        ob_ref[...] = b_ref[...]

    @pl.when(jnp.logical_not(idle))
    def _():
        def store(r, s, value):
            if s >= h - r:
                oa_ref[idx_a(h, r, s)] = value
            else:
                ob_ref[idx_b(h, r, s)] = value

        upper_blocks(h, flags_ref, ra_ref, sa_ref, sb_ref, a_ref, b_ref, l_ref, store)


def lower_blocks(h, flags_ref, ra_ref, rb_ref, sl_ref, a_ref, b_ref, l_ref, store, wanted):
    width = 2 * h + 1

    def above(t, s):
        if t >= 0:
            return a_ref[idx_a(h, t, s)] if s >= h - t else b_ref[idx_b(h, t, s)]
        t = t + h
        return ra_ref[idx_a(h, t, s)] if s >= h - t else rb_ref[idx_b(h, t, s)]

    for r in range(h):
        for k in range(h):
            if not wanted(r, k):
                continue
            flag = flags_ref[r * width + k]

            @pl.when(flag != 0)
            def _(r=r, k=k):
                reach = range(h - k, h + 1)
                pivot = above(r - h + k, 0)
                left = [l_ref[r * h + h - m] for m in reach]
                right = [strict_upper(pivot)] + [above(r - m, k - h + m) for m in reach[1:]]
                rest = sl_ref[r * h + k].astype(jnp.float32) - jnp.dot(
                    jnp.concatenate(left, axis=1),
                    jnp.concatenate(right, axis=0),
                    preferred_element_type=jnp.float32,
                )
                store(r, k, (rest * (1.0 / take_diag(pivot))).astype(jnp.bfloat16))

            @pl.when(flag == 0)
            def _(r=r, k=k):
                store(r, k, jnp.zeros(sl_ref.shape[1:], jnp.bfloat16))


def lower_kernel(h, flags_ref, ra_ref, rb_ref, sl_ref, a_ref, b_ref, l_ref, o_ref):
    @pl.when(flags_ref[h * (2 * h + 1)] == 0)
    def _():
        o_ref[...] = l_ref[...]

    @pl.when(flags_ref[h * (2 * h + 1)] != 0)
    def _():
        def store(r, k, value):
            o_ref[r * h + k] = value

        lower_blocks(
            h, flags_ref, ra_ref, rb_ref, sl_ref, a_ref, b_ref, l_ref, store, lambda r, k: True
        )


def middle_kernel(h, flags_ref, ra_ref, sa_ref, sb_ref, sl_ref, a_ref, b_ref, l_ref, o_ref):
    idle = flags_ref[h * (2 * h + 1)] == 0

    @pl.when(idle)
    def _():
        for n, (t, s) in enumerate(list_a(h)):
            o_ref[t, h + s] = a_ref[n]
        for n, (t, s) in enumerate(list_b(h)):
            o_ref[t, h + s] = b_ref[n]
        for t in range(h):
            for k in range(h):
                o_ref[t, k] = l_ref[t * h + k]

    @pl.when(jnp.logical_not(idle))
    def _():
        def store_upper(r, s, value):
            o_ref[r, h + s] = value

        def store(r, k, value):
            o_ref[r, k] = value

        def wanted(r, k):
            return k >= h - r

        for t in range(h):
            for k in range(h - t):
                o_ref[t, k] = jnp.zeros(o_ref.shape[2:], o_ref.dtype)
        upper_blocks(h, flags_ref, ra_ref, sa_ref, sb_ref, a_ref, b_ref, l_ref, store_upper)
        lower_blocks(
            h, flags_ref, ra_ref, None, sl_ref, a_ref, b_ref, l_ref, store, wanted
        )


def last_kernel(h, flags_ref, rb_ref, sl_ref, l_ref, out_in_ref, o_ref, buf_ref, sems):
    del out_in_ref

    @pl.when(flags_ref[h * (2 * h + 1)] != 0)
    def _():
        entries = [(r, k) for r in range(h) for k in range(h - r)]

        def copy(n):
            r, k = entries[n]
            return pltpu.make_async_copy(buf_ref.at[n], o_ref.at[r, k], sems.at[n])

        def store(r, k, value):
            buf_ref[entries.index((r, k))] = value

        for n, entry in enumerate(entries):
            lower_blocks(
                h, flags_ref, None, rb_ref, sl_ref, None, None, l_ref, store,
                lambda r, k, entry=entry: (r, k) == entry,
            )
            copy(n).start()
        for n in range(len(entries)):
            copy(n).wait()


def call(body, outs, name, products, smem_first=True):
    specs = [pl.BlockSpec(memory_space=pltpu.SMEM)] if smem_first else []

    def run(*args):
        vmem = [pl.BlockSpec(memory_space=pltpu.VMEM)] * (len(args) - len(specs))
        block = outs[0].shape[-1]
        nbytes = sum(x.size * x.dtype.itemsize for x in list(args) + list(outs))
        return pl.pallas_call(
            body,
            out_shape=outs,
            in_specs=specs + vmem,
            out_specs=[pl.BlockSpec(memory_space=pltpu.VMEM)] * len(outs),
            compiler_params=pltpu.CompilerParams(vmem_limit_bytes=48 * 1024 * 1024),
            cost_estimate=pl.CostEstimate(
                flops=2 * products * block**3, bytes_accessed=nbytes, transcendentals=0
            ),
            name=name,
        )(*args)

    return run


def per_device(blocks, diag_shift, offsets):
    rows, width, size, _ = blocks.shape
    h = (width - 1) // 2
    groups = lax.axis_size("grp")
    devices = lax.axis_size("slab") * groups
    assert rows == h and groups >= 3
    grp = lax.axis_index("grp")
    device = lax.axis_index("slab") * groups + grp
    pairs = [(i, i + 1) for i in range(devices - 1)]
    bf = jnp.bfloat16
    half = h * (h + 1) // 2
    pack = jax.ShapeDtypeStruct((half, size, size), bf)
    lows = jax.ShapeDtypeStruct((h * h, size, size), bf)

    first_pairs = [p for p in pairs if p[1] % groups != 0]
    own_values, raw_a, raw_b = pl.pallas_call(
        functools.partial(pack_kernel, h),
        grid=(1,),
        in_specs=[pl.BlockSpec((rows * size,), lambda i: (0,))]
        + [
            pl.BlockSpec((rows, 1, size, size), functools.partial(lambda k, i: (0, k, 0, 0), h + s))
            for s in range(h + 1)
        ],
        out_specs=[
            pl.BlockSpec((rows, size), lambda i: (0, 0)),
            pl.BlockSpec((half, size, size), lambda i: (0, 0, 0)),
            pl.BlockSpec((half, size, size), lambda i: (0, 0, 0)),
        ],
        out_shape=[jax.ShapeDtypeStruct((rows, size), jnp.float32), pack, pack],
        name="pack",
    )(diag_shift, *([blocks] * (h + 1)))
    reach_up = jnp.broadcast_to(offsets[:, 1:2].astype(jnp.float32), (rows, 128))
    small = jnp.concatenate([own_values, reach_up], 1)
    before = lax.ppermute(small, AXES, pairs)
    after = lax.ppermute(own_values, AXES, [(j, i) for i, j in pairs])
    halo_a = lax.ppermute(raw_a, AXES, first_pairs)
    halo_b = lax.ppermute(raw_b, AXES, first_pairs)

    widened = jnp.concatenate([before[:, :size], own_values, after], 0)
    positive = widened > 0
    scales = jnp.where(positive, 1.0 / jnp.sqrt(jnp.where(positive, widened, 1.0)), 0.0)
    scales_t = scales.T

    all_rows = rows * devices
    row_ids = device * rows + jnp.arange(rows, dtype=jnp.int32)
    relative = jnp.arange(width, dtype=jnp.int32) - h
    target = row_ids[:, None] + relative[None, :]
    left_side = (relative < 0) & (-relative <= offsets[:, 0:1]) & (target >= 0)
    right_side = (relative > 0) & (relative <= offsets[:, 1:2]) & (target < all_rows)
    present = ((relative == 0) | left_side | right_side).astype(jnp.int32).reshape(-1)
    steps = jnp.arange(h + 1, dtype=jnp.int32)
    before_reach = before[:, size : size + 1].astype(jnp.int32)
    before_target = row_ids[:, None] - rows + steps[None, :]
    before_present = (steps == 0) | ((steps <= before_reach) & (before_target < all_rows))
    before_present = before_present.astype(jnp.int32).reshape(-1)

    sa, sb, sl = call(functools.partial(scale_own_kernel, h), [pack, pack, lows], "scale", 1)(
        present, blocks, widened, scales, scales_t
    )
    (ra,) = call(functools.partial(scale_recv_kernel, h, list_a(h)), [pack], "scale_a", 1)(
        before_present, halo_a, widened, scales, scales_t
    )
    (rb,) = call(functools.partial(scale_recv_kernel, h, list_b(h)), [pack], "scale_b", 1)(
        before_present, halo_b, widened, scales, scales_t
    )

    def flags(active):
        return jnp.concatenate([present, active.astype(jnp.int32).reshape(1)])

    upper = call(functools.partial(upper_kernel, h), [pack, pack], "upper", 30)
    lower = call(functools.partial(lower_kernel, h), [lows], "lower", 20)
    full = jax.ShapeDtypeStruct(blocks.shape, bf)
    middle = call(functools.partial(middle_kernel, h), [full], "middle", 50)
    vmem = pl.BlockSpec(memory_space=pltpu.VMEM)
    anywhere = pl.BlockSpec(memory_space=pl.ANY)
    last = pl.pallas_call(
        functools.partial(last_kernel, h),
        out_shape=full,
        in_specs=[pl.BlockSpec(memory_space=pltpu.SMEM), vmem, vmem, vmem, anywhere],
        out_specs=anywhere,
        scratch_shapes=[pltpu.VMEM((half, size, size), bf), pltpu.SemaphoreType.DMA((half,))],
        input_output_aliases={4: 0},
        compiler_params=pltpu.CompilerParams(vmem_limit_bytes=32 * 1024 * 1024),
        cost_estimate=pl.CostEstimate(
            flops=20 * size**3, bytes_accessed=blocks.size, transcendentals=0
        ),
        name="last",
    )

    on = flags(grp > 0)
    a1, b1 = upper(on, ra, sa, sb, sa, sb, sl)
    second_pairs = [p for p in pairs if p[1] % groups != 1]
    ra1 = lax.ppermute(a1, AXES, second_pairs)
    rb1 = lax.ppermute(b1, AXES, second_pairs)
    (l1,) = lower(on, ra, rb, sl, sa, sb, sl)

    on = flags(grp != 1)
    a2, b2 = upper(on, ra1, sa, sb, a1, b1, l1)
    third_pairs = [p for p in pairs if p[1] % groups < 2]
    ra2 = lax.ppermute(a2, AXES, third_pairs)
    rb2 = lax.ppermute(b2, AXES, third_pairs)
    (l2,) = lower(on, ra1, rb1, sl, a1, b1, l1)

    on = flags(grp < 2)
    (out,) = middle(on, ra2, sa, sb, sl, a2, b2, l2)
    out = last(on, rb2, sl, l2, out)
    return out


def solution(mesh):
    return jax.shard_map(
        per_device,
        mesh=mesh,
        in_specs=(
            P(AXES, None, None, None),
            P(AXES),
            P(AXES, None),
        ),
        out_specs=P(AXES, None, None, None),
        check_vma=False,
    )
```
